64 devices in a mesh: dp: 4 (over x, y), ep: 16 (over z, core).
Axes of the slice: x: 2, y: 2, z: 8, core: 2. Of those that a mesh axis runs over, the one named last changes fastest.
The devices are a block of a 4x4x8 slice.
Arguments:
- x_disp: bfloat16 [64, 32, 96, 1024], P('dp', 'ep'), parts along dimension 0
- w_gate: bfloat16 [32, 1024, 512], P('ep')
- w_up: bfloat16 [32, 1024, 512], P('ep')
- w_down: bfloat16 [32, 512, 1024], P('ep')
- d_out: bfloat16 [12288, 1024], P(('dp', 'ep')), parts along dimension 0
- slot_idx: int32 [12288, 8], P(('dp', 'ep')), parts along dimension 0
- expert_id: int32 [12288, 8], P(('dp', 'ep')), parts along dimension 0
- gate_wt: float32 [12288, 8], P(('dp', 'ep')), parts along dimension 0
Outputs:
- output 1: bfloat16 [64, 32, 96, 1024], P('dp', 'ep'), parts along dimension 0
- output 2: bfloat16 [128, 1024, 512], P(('dp', 'ep')), parts along dimension 0
- output 3: bfloat16 [128, 1024, 512], P(('dp', 'ep')), parts along dimension 0
- output 4: bfloat16 [128, 512, 1024], P(('dp', 'ep')), parts along dimension 0
- output 5: float32 [12288, 8], P(('dp', 'ep')), parts along dimension 0
There are 4 independent parts. The reference program is written for one: setup_inputs(seed, part) draws one part's arguments, and reference() takes and returns one part's arrays. A program takes and returns all parts, laid end to end along the dimension named above; an argument that names none is the same for every part.
All inputs are finite; a program needn't handle non-finite values.
Results may differ from the reference program's by a relative error of at most 0.00498987.
Values are sent between devices in bfloat16 or wider.
A program may use at most 768 MiB of HBM per device.

```python
import jax
import jax.numpy as jnp
from jax import lax

GROUP_SIZE = 16
TOK_DEV = 192
TOP_K = 8
EXPERTS = 32
MODEL_DIM = 1024
FFN_DIM = 512
CAPACITY = 96

TOKENS = GROUP_SIZE * TOK_DEV
SLOT_COUNT = EXPERTS * CAPACITY
PER_SOURCE = TOK_DEV * TOP_K


def draw_routes(key):
    key_noise, key_tilt, key_hot = jax.random.split(key, 3)
    noise_int = jax.random.randint(key_noise, (TOKENS, EXPERTS), 0, 4096)
    tilt_int = jax.random.permutation(key_tilt, EXPERTS) * (1024 // EXPERTS)
    hot_expert = jax.random.randint(key_hot, (), 0, EXPERTS)
    expert_ids = jnp.arange(EXPERTS)[None, :]
    even_tok = (jnp.arange(TOKENS) % 2 == 0)[:, None]
    bonus_int = jnp.where(even_tok & (expert_ids == hot_expert), 1048576, 0)
    scores = (noise_int + tilt_int[None, :] + bonus_int) * EXPERTS + expert_ids
    expert_id = lax.top_k(scores, TOP_K)[1].astype(jnp.int32)
    picked = jnp.zeros((TOKENS, EXPERTS), jnp.int32).at[jnp.arange(TOKENS)[:, None], expert_id].add(1)
    picked = picked.reshape(GROUP_SIZE, TOK_DEV, EXPERTS)
    earlier = jnp.cumsum(picked, axis=1) - picked
    order_pos = jnp.take_along_axis(earlier, expert_id.reshape(GROUP_SIZE, TOK_DEV, TOP_K), axis=2)
    slot_idx = jnp.where(order_pos < CAPACITY, order_pos, -1).reshape(TOKENS, TOP_K).astype(jnp.int32)
    return slot_idx, expert_id


def setup_inputs(seed: int = 0, part: int = 0) -> dict:
    base_key = jax.random.key(seed)
    part_key = jax.random.fold_in(base_key, part)
    key_x, key_out, key_gate, key_route = jax.random.split(part_key, 4)
    key_wg, key_wu, key_wd = jax.random.split(jax.random.key(seed + 1), 3)
    x_disp = jax.random.normal(key_x, (GROUP_SIZE, EXPERTS, CAPACITY, MODEL_DIM), jnp.float32).astype(jnp.bfloat16)
    w_gate = (jax.random.normal(key_wg, (EXPERTS, MODEL_DIM, FFN_DIM), jnp.float32) * MODEL_DIM ** -0.5).astype(jnp.bfloat16)
    w_up = (jax.random.normal(key_wu, (EXPERTS, MODEL_DIM, FFN_DIM), jnp.float32) * MODEL_DIM ** -0.5).astype(jnp.bfloat16)
    w_down = (jax.random.normal(key_wd, (EXPERTS, FFN_DIM, MODEL_DIM), jnp.float32) * FFN_DIM ** -0.5).astype(jnp.bfloat16)
    d_out = jax.random.normal(key_out, (TOKENS, MODEL_DIM), jnp.float32).astype(jnp.bfloat16)
    slot_idx, expert_id = draw_routes(key_route)
    gate_wt = jax.random.uniform(key_gate, (TOKENS, TOP_K), jnp.float32, 0.05, 1.0)
    return {'x_disp': x_disp, 'w_gate': w_gate, 'w_up': w_up, 'w_down': w_down, 'd_out': d_out, 'slot_idx': slot_idx, 'expert_id': expert_id, 'gate_wt': gate_wt}


def one_expert(operands):
    x_rows, out_rows, d_slot, w_gate, w_up, w_down = operands
    pre_gate = jnp.dot(x_rows, w_gate, preferred_element_type=jnp.float32)
    pre_up = jnp.dot(x_rows, w_up, preferred_element_type=jnp.float32)
    gate_sig = jax.nn.sigmoid(pre_gate)
    silu_gate = pre_gate * gate_sig
    hidden = (silu_gate * pre_up).astype(jnp.bfloat16)
    y_rows = jnp.dot(hidden, w_down, preferred_element_type=jnp.float32).astype(jnp.bfloat16)
    grad_hidden = jnp.dot(d_slot, w_down.T, preferred_element_type=jnp.float32).astype(jnp.bfloat16).astype(jnp.float32)
    grad_pre_gate = (grad_hidden * pre_up * gate_sig * (1.0 + pre_gate * (1.0 - gate_sig))).astype(jnp.bfloat16)
    grad_pre_up = (grad_hidden * silu_gate).astype(jnp.bfloat16)
    grad_x = (jnp.dot(grad_pre_gate, w_gate.T, preferred_element_type=jnp.float32) + jnp.dot(grad_pre_up, w_up.T, preferred_element_type=jnp.float32)).astype(jnp.bfloat16)
    grad_w_gate = jnp.dot(x_rows.T, grad_pre_gate, preferred_element_type=jnp.float32).astype(jnp.bfloat16)
    grad_w_up = jnp.dot(x_rows.T, grad_pre_up, preferred_element_type=jnp.float32).astype(jnp.bfloat16)
    grad_w_down = jnp.dot(hidden.T, d_slot, preferred_element_type=jnp.float32).astype(jnp.bfloat16)
    gate_grad_rows = jnp.sum(out_rows.astype(jnp.float32) * y_rows.astype(jnp.float32), axis=1)
    return grad_x, grad_w_gate, grad_w_up, grad_w_down, gate_grad_rows


def by_expert(arr):
    return jnp.moveaxis(arr.reshape(GROUP_SIZE, EXPERTS, CAPACITY, MODEL_DIM), 1, 0).reshape(EXPERTS, GROUP_SIZE * CAPACITY, MODEL_DIM)


def owners(pos_row):
    return jnp.full((SLOT_COUNT,), PER_SOURCE, jnp.int32).at[pos_row].set(jnp.arange(PER_SOURCE, dtype=jnp.int32), mode='drop')


def pick_rows(tok_rows, gate_row, owner_row):
    rows_out = jnp.take(tok_rows, owner_row // TOP_K, axis=0, mode='fill', fill_value=0)
    gates_out = jnp.take(gate_row, owner_row, mode='fill', fill_value=0)
    return rows_out, gates_out


def take_fill(values, index_row):
    return jnp.take(values, index_row, mode='fill', fill_value=0)


def reference(x_disp, w_gate, w_up, w_down, d_out, slot_idx, expert_id, gate_wt):
    flat_pos = jnp.where(slot_idx >= 0, expert_id * CAPACITY + slot_idx, SLOT_COUNT).reshape(GROUP_SIZE, PER_SOURCE)
    owner_ids = jax.vmap(owners)(flat_pos)
    out_rows, gate_rows = jax.vmap(pick_rows)(d_out.reshape(GROUP_SIZE, TOK_DEV, MODEL_DIM), gate_wt.reshape(GROUP_SIZE, PER_SOURCE), owner_ids)
    d_slot = (out_rows.astype(jnp.float32) * gate_rows[:, :, None]).astype(jnp.bfloat16)
    results = lax.map(one_expert, (by_expert(x_disp), by_expert(out_rows), by_expert(d_slot), w_gate, w_up, w_down))
    grad_x, grad_w_gate, grad_w_up, grad_w_down, gate_grad_rows = results
    grad_x_disp = jnp.moveaxis(grad_x.reshape(EXPERTS, GROUP_SIZE, CAPACITY, MODEL_DIM), 0, 1)
    gate_grad_src = jnp.moveaxis(gate_grad_rows.reshape(EXPERTS, GROUP_SIZE, CAPACITY), 0, 1).reshape(GROUP_SIZE, SLOT_COUNT)
    grad_gate = jax.vmap(take_fill)(gate_grad_src, flat_pos).reshape(TOKENS, TOP_K)
    return grad_x_disp, grad_w_gate, grad_w_up, grad_w_down, grad_gate
```

```python
import functools

import jax
import jax.numpy as jnp
from jax import lax
from jax.experimental import pallas as pl
from jax.experimental.pallas import tpu as pltpu
from jax.sharding import PartitionSpec as P

F32 = jnp.float32
BF16 = jnp.bfloat16
MXU = 256


def dot(a, b, ca, cb):
    return lax.dot_general(a, b, (((ca,), (cb,)), ((), ())), preferred_element_type=F32)


def peers(n):
    me = lax.axis_index('ep')
    chips = n // 2
    z, core = me // 2, me % 2
    sgn = 1 - 2 * core
    sib = z * 2 + 1 - core
    nxt = ((z + sgn + chips) % chips) * 2 + core

    def src(k):
        p, side = k // 2, k % 2
        dist, blk = (p + 1) // 2, (p + 1) % 2
        chip = (z + chips - sgn * (1 - 2 * side) * dist) % chips
        other = (side + blk) % 2
        ring_core = jnp.where(p == 0, (core + side) % 2, (core + other) % 2)
        return chip * 2 + ring_core

    return me, sib, nxt, src


def main_kernel(n, x_hbm, wg_hbm, wu_hbm, wd_hbm, do_hbm, slot_ref, eid_ref, gate_ref,
                ybuf, wgu, wd, gg_out,
                gbuf, xbuf, pbuf, qbuf, hbuf, dab, acc_gu, acc_d, rt_src, rt_dst, gg_src, gg_dst,
                x_sem, w_sem, g_sem, ring_s, ring_r, sib_s, sib_r, own_s, own_r,
                rt_s, rt_r, gg_s, gg_r):
    e_loc, cap, dim = x_hbm.shape[1], x_hbm.shape[2], x_hbm.shape[3]
    ffn = wd_hbm.shape[1]
    tok = do_hbm.shape[0]
    half = tok // 2
    rows = n * cap
    pairs = n // 2
    steps = 2 * (pairs - 1)
    me, sib, nxt, src = peers(n)

    def remote(s, d, ss, rs, dev):
        return pltpu.make_async_remote_copy(src_ref=s, dst_ref=d, send_sem=ss, recv_sem=rs,
                                            device_id={'ep': dev}, device_id_type=pl.DeviceIdType.MESH)

    barrier = pltpu.get_barrier_semaphore()

    @pl.loop(1, n)
    def _(i):
        pl.semaphore_signal(barrier, inc=1, device_id={'ep': (me + i) % n}, device_id_type=pl.DeviceIdType.MESH)

    own_load = pltpu.make_async_copy(do_hbm, gbuf.at[0], g_sem)
    own_load.start()

    def x_load(k):
        r = pl.ds(pl.multiple_of(k * cap, 32), cap)
        return pltpu.make_async_copy(x_hbm.at[src(k)], xbuf.at[:, r, :], x_sem.at[k])

    def w_loads(e):
        return (pltpu.make_async_copy(wg_hbm.at[e], wgu.at[e, :, pl.ds(0, ffn)], w_sem.at[e, 0]),
                pltpu.make_async_copy(wu_hbm.at[e], wgu.at[e, :, pl.ds(ffn, ffn)], w_sem.at[e, 1]),
                pltpu.make_async_copy(wd_hbm.at[e], wd.at[e], w_sem.at[e, 2]))

    tile_src = 4
    for k in range(tile_src):
        x_load(k).start()
    for e in range(e_loc):
        for c in w_loads(e):
            c.start()
    for k in range(tile_src, n):
        x_load(k).start()

    slot1 = slot_ref[...].astype(F32) + 1.0
    eid = eid_ref[...]
    gate = gate_ref[...]
    for e in range(n * e_loc):
        hit = eid == e
        rt_src[e // e_loc, pl.ds(e % e_loc, 1), :] = jnp.sum(jnp.where(hit, slot1, 0.0), axis=0, keepdims=True) - 1.0
        rt_src[e // e_loc, pl.ds(e_loc + e % e_loc, 1), :] = jnp.sum(jnp.where(hit, gate, 0.0), axis=0, keepdims=True)

    own_load.wait()
    pl.semaphore_wait(barrier, n - 1)

    def chunk(k, m):
        return gbuf.at[k, pl.ds(pl.multiple_of((m % 2) * half, 32), half), :]

    def ring_copy(m, k_from):
        return remote(chunk(k_from, m), chunk(2 + 2 * (m // 2), m), ring_s.at[m], ring_r.at[m], nxt)

    def sib_copy(m):
        k = 2 + 2 * (m // 2)
        return remote(chunk(k, m), chunk(k + 1, m), sib_s.at[m], sib_r.at[m], sib)

    own_copy = remote(gbuf.at[0], gbuf.at[1], own_s, own_r, sib)
    for m in range(2):
        ring_copy(m, 0).start()
    own_copy.start()

    def comm(m):
        k = 2 + 2 * (m // 2)
        ring_copy(m, k).wait_recv()
        if isinstance(m, int):
            if m + 4 < steps:
                ring_copy(m + 4, k).start()
        else:
            @pl.when(m + 4 < steps)
            def _():
                ring_copy(m + 4, k).start()
        sib_copy(m).start()

    def route_copy(i):
        return remote(rt_src.at[(me + i) % n], rt_dst.at[me], rt_s.at[i], rt_r.at[i], (me + i) % n)

    tile = tile_src * cap
    n_tiles = rows // tile

    def phase_a(e, t):
        r = pl.ds(pl.multiple_of(t * tile, 128), tile)
        xt = xbuf[e, r, :]
        for c in range(ffn // MXU):
            cols = pl.ds(c * MXU, MXU)
            a = dot(xt, wgu[e, :, cols], 1, 0)
            b = dot(xt, wgu[e, :, pl.ds(ffn + c * MXU, MXU)], 1, 0)
            sg = jax.nn.sigmoid(a)
            silu = a * sg
            hbuf[e, r, cols] = (silu * b).astype(BF16)
            qbuf[e, r, cols] = silu
            pbuf[e, r, cols] = b * sg * (1.0 + a * (1.0 - sg))
        ht = hbuf[e, r, :]
        for c in range(dim // MXU):
            cols = pl.ds(c * MXU, MXU)
            ybuf[e, r, cols] = dot(ht, wd[e, :, cols], 1, 0).astype(BF16)

    def a_step(i):
        e, t = i % e_loc, i // e_loc

        @pl.when(e == 0)
        def _():
            for j in range(tile_src):
                x_load(t * tile_src + j).wait()

        @pl.when(t == 0)
        def _():
            for c in w_loads(e):
                c.wait()

        phase_a(e, t)

    a_step(0)
    own_copy.wait_recv()
    for m in range(2, 4):
        ring_copy(m, 1).start()

    @pl.loop(1, n)
    def _(i):
        route_copy(i).start()
    rt_dst[me] = rt_src[me]

    @pl.loop(1, n_tiles * e_loc)
    def _(i):
        a_step(i)

        @pl.when(i % 3 != 0)
        def _():
            comm((2 * i - 1) // 3)
    done_m = (2 * (n_tiles * e_loc - 1) - 1) // 3 + 1

    @pl.loop(1, n)
    def _(i):
        route_copy(i).wait_recv()

    slot_no = lax.broadcasted_iota(jnp.int32, (cap, tok), 0).astype(F32)

    def select_rows(k):
        s = src(k)
        r = pl.ds(pl.multiple_of(k * cap, 32), cap)
        rt = rt_dst[s]
        hits = [slot_no == rt[e:e + 1, :] for e in range(e_loc)]
        gcols = [jnp.sum(jnp.where(hits[e], rt[e_loc + e:e_loc + e + 1, :], 0.0), axis=1, keepdims=True)
                 for e in range(e_loc)]
        onehot = jnp.concatenate([jnp.where(h, 1.0, 0.0).astype(BF16) for h in hits], axis=0)
        dots = [jnp.zeros((cap, 1), F32) for _ in range(e_loc)]
        for c in range(dim // MXU):
            cols = pl.ds(c * MXU, MXU)
            o = dot(onehot, gbuf[k, :, cols], 1, 0)
            for e in range(e_loc):
                oe = o[e * cap:(e + 1) * cap, :]
                dots[e] = dots[e] + jnp.sum(oe * ybuf[e, r, cols].astype(F32), axis=1, keepdims=True)
                ybuf[e, r, cols] = (oe * gcols[e]).astype(BF16)
        for e in range(e_loc):
            gg_src[k, pl.ds(e, 1), :] = jnp.sum(jnp.where(hits[e], dots[e], 0.0), axis=0, keepdims=True)

    def gg_copy(k):
        s = src(k)
        off = (s - me + n) % n
        return remote(gg_src.at[k], gg_dst.at[me], gg_s.at[off], gg_r.at[off], s)

    def gg_send(k0, k1):
        for k in range(k0, k1):
            if k == 0:
                gg_dst[me] = gg_src[0]
            else:
                gg_copy(k).start()

    def hidden_grads(e, r0, r1):
        r = pl.ds(r0, r1 - r0)
        dy = ybuf[e, r, :]
        for c in range(ffn // MXU):
            cols = pl.ds(c * MXU, MXU)
            dh = dot(dy, wd[e, cols, :], 1, 1).astype(BF16).astype(F32)
            dab[e, r, cols] = (dh * pbuf[e, r, cols]).astype(BF16)
            dab[e, r, pl.ds(ffn + c * MXU, MXU)] = (dh * qbuf[e, r, cols]).astype(BF16)

    def weight_grad(lhs, rhs, acc, out, w0, w1, e, t):
        cols = pl.ds(pl.multiple_of(t * MXU, MXU), MXU)
        r = pl.ds(w0, w1 - w0)
        for c in range(dim // (2 * MXU)):
            oc = pl.ds(c * 2 * MXU, 2 * MXU)
            g = dot(lhs[e, r, cols], rhs[e, r, oc], 0, 0)
            if w0 > 0:
                g = g + acc[e, cols, oc]
            if w1 == rows:
                out[e, cols, oc] = g.astype(BF16)
            else:
                acc[e, cols, oc] = g

    def x_grad(e, r0, r1):
        r = pl.ds(r0, r1 - r0)
        da = dab[e, r, :]
        for c in range(dim // MXU):
            ybuf[e, r, pl.ds(c * MXU, MXU)] = dot(da, wgu[e, pl.ds(c * MXU, MXU), :], 1, 1).astype(BF16)

    next_m = [done_m]

    def comm_next(count=1):
        for _ in range(count):
            if next_m[0] < steps:
                comm(next_m[0])
                next_m[0] += 1

    stages = [(0, 3, 0, 512), (3, 5, 512, 768), (5, 7, 768, 1280), (7, 8, 1280, 1536)]
    for p0, p1, w0, w1 in stages:
        need = 2 * (p1 - 1)
        if next_m[0] < need:
            comm_next(need - next_m[0])
        for p in range(max(p0, 1), p1):
            for m in (2 * p - 2, 2 * p - 1):
                sib_copy(m).wait_recv()

        @pl.loop(2 * p0, 2 * p1)
        def _(k):
            select_rows(k)
        comm_next()

        @pl.loop(0, e_loc)
        def _(e):
            hidden_grads(e, 2 * p0 * cap, 2 * p1 * cap)
        gg_send(2 * p0, 2 * p1)
        comm_next()

        @pl.loop(0, e_loc * (ffn // MXU))
        def _(i):
            weight_grad(hbuf, ybuf, acc_d, wd, w0, w1, i % e_loc, i // e_loc)
        comm_next()

        @pl.loop(0, e_loc)
        def _(e):
            x_grad(e, w0, w1)
        comm_next()

        @pl.loop(0, e_loc * (dim // MXU))
        def _(i):
            weight_grad(xbuf, dab, acc_gu, wgu, w0, w1, i % e_loc, i // e_loc)
        comm_next()

    @pl.loop(1, n)
    def _(k):
        gg_copy(k).wait_recv()
        gg_copy(k).wait_send()
        route_copy(k).wait_send()
    for m in range(steps):
        ring_copy(m, 0).wait_send()
        sib_copy(m).wait_send()
    own_copy.wait_send()
    gg_out[...] = gg_dst[...]


def write_kernel(n, ybuf, wgu, wd, gg, eid_ref, gx_hbm, gwg_hbm, gwu_hbm, gwd_hbm, gate_out, y_sem, w_sem):
    cap = gx_hbm.shape[2]
    e_loc, ffn = wd.shape[0], wd.shape[1]
    _, _, _, src = peers(n)
    copies = [pltpu.make_async_copy(wgu.at[:, :, pl.ds(0, ffn)], gwg_hbm, w_sem.at[0]),
              pltpu.make_async_copy(wgu.at[:, :, pl.ds(ffn, ffn)], gwu_hbm, w_sem.at[1]),
              pltpu.make_async_copy(wd, gwd_hbm, w_sem.at[2])]
    for k in range(n):
        copies.append(pltpu.make_async_copy(ybuf.at[:, pl.ds(k * cap, cap), :], gx_hbm.at[src(k)], y_sem.at[k]))
    for c in copies:
        c.start()
    eid = eid_ref[...]
    out = jnp.zeros(eid.shape, F32)
    for e in range(n * e_loc):
        out = out + jnp.where(eid == e, gg[e // e_loc, pl.ds(e % e_loc, 1), :], 0.0)
    gate_out[...] = out
    for c in copies:
        c.wait()


def solution(mesh):
    n = mesh.shape['ep']

    def local_step(x_disp, w_gate, w_up, w_down, d_out, slot_idx, expert_id, gate_wt):
        _, e_loc, cap, dim = x_disp.shape
        ffn = w_down.shape[1]
        tok, top_k = slot_idx.shape
        rows = n * cap
        steps = 2 * (n // 2 - 1)
        slot_t, eid_t, gate_t = slot_idx.T, expert_id.T, gate_wt.T
        vmem = pl.BlockSpec(memory_space=pltpu.VMEM)
        hbm = pl.BlockSpec(memory_space=pl.ANY)
        dma = pltpu.SemaphoreType.DMA
        ybuf, wgu, wd, gg = pl.pallas_call(
            functools.partial(main_kernel, n),
            out_shape=(pltpu.VMEM((e_loc, rows, dim), BF16),
                       pltpu.VMEM((e_loc, dim, 2 * ffn), BF16),
                       pltpu.VMEM((e_loc, ffn, dim), BF16),
                       pltpu.VMEM((n, e_loc, tok), F32)),
            in_specs=[hbm] * 5 + [vmem] * 3,
            out_specs=[vmem] * 4,
            scratch_shapes=[
                pltpu.VMEM((n, tok, dim), BF16),
                pltpu.VMEM((e_loc, rows, dim), BF16),
                pltpu.VMEM((e_loc, rows, ffn), F32),
                pltpu.VMEM((e_loc, rows, ffn), F32),
                pltpu.VMEM((e_loc, rows, ffn), BF16),
                pltpu.VMEM((e_loc, rows, 2 * ffn), BF16),
                pltpu.VMEM((e_loc, dim, 2 * ffn), F32),
                pltpu.VMEM((e_loc, ffn, dim), F32),
                pltpu.VMEM((n, 2 * e_loc, tok), F32),
                pltpu.VMEM((n, 2 * e_loc, tok), F32),
                pltpu.VMEM((n, e_loc, tok), F32),
                pltpu.VMEM((n, e_loc, tok), F32),
                dma((n,)), dma((e_loc, 3)), dma,
                dma((steps,)), dma((steps,)), dma((steps,)), dma((steps,)), dma, dma,
                dma((n,)), dma((n,)), dma((n,)), dma((n,)),
            ],
            compiler_params=pltpu.CompilerParams(collective_id=0, has_side_effects=True,
                                                 vmem_limit_bytes=49 * 1024 * 1024),
            name='experts',
        )(x_disp, w_gate, w_up, w_down, d_out, slot_t, eid_t, gate_t)
        grad_x, grad_wg, grad_wu, grad_wd, gate_out = pl.pallas_call(
            functools.partial(write_kernel, n),
            out_shape=(jax.ShapeDtypeStruct(x_disp.shape, BF16),
                       jax.ShapeDtypeStruct(w_gate.shape, BF16),
                       jax.ShapeDtypeStruct(w_up.shape, BF16),
                       jax.ShapeDtypeStruct(w_down.shape, BF16),
                       jax.ShapeDtypeStruct((top_k, tok), F32)),
            in_specs=[vmem] * 5,
            out_specs=[hbm] * 4 + [vmem],
            scratch_shapes=[dma((n,)), dma((3,))],
            compiler_params=pltpu.CompilerParams(vmem_limit_bytes=4 * 1024 * 1024),
            name='write_out',
        )(ybuf, wgu, wd, gg, eid_t)
        return grad_x, grad_wg, grad_wu, grad_wd, gate_out.T

    token_place = P(('dp', 'ep'), None)
    weight_place = P('ep', None, None)
    slot_place = P('dp', 'ep', None, None)
    grad_place = P(('dp', 'ep'), None, None)
    return jax.shard_map(local_step, mesh=mesh,
                         in_specs=(slot_place, weight_place, weight_place, weight_place,
                                   token_place, token_place, token_place, token_place),
                         out_specs=(slot_place, grad_place, grad_place, grad_place, token_place),
                         check_vma=False)
```

```python
import functools

import jax
import jax.numpy as jnp
from jax import lax
from jax.experimental import pallas as pl
from jax.experimental.pallas import tpu as pltpu
from jax.sharding import PartitionSpec as P

F32 = jnp.float32
BF16 = jnp.bfloat16
MXU = 256
LANES = 128


def dot(a, b, ca, cb):
    return lax.dot_general(a, b, (((ca,), (cb,)), ((), ())), preferred_element_type=F32)


def peers(n):
    me = lax.axis_index('ep')
    chips = n // 2
    z, core = me // 2, me % 2
    sgn = 1 - 2 * core
    sib = z * 2 + 1 - core
    nxt = ((z + sgn + chips) % chips) * 2 + core

    def src(k):
        p, side = k // 2, k % 2
        dist, blk = (p + 1) // 2, (p + 1) % 2
        chip = (z + chips - sgn * (1 - 2 * side) * dist) % chips
        other = (side + blk) % 2
        ring_core = jnp.where(p == 0, (core + side) % 2, (core + other) % 2)
        return chip * 2 + ring_core

    return me, sib, nxt, src


def main_kernel(n, x_hbm, wg_hbm, wu_hbm, wd_hbm, do_hbm, slot_ref, eid_ref, gate_ref,
                ybuf, xbuf, wgu, wd, dab, gg_out,
                gbuf, pbuf, qbuf, hbuf, acc_gu, acc_d, rt_src, rt_dst, gg_src, gg_dst,
                x_sem, w_sem, g_sem, ring_s, ring_r, sib_s, sib_r, own_s, own_r,
                rt_s, rt_r, gg_s, gg_r):
    e_loc, cap, dim = x_hbm.shape[1], x_hbm.shape[2], x_hbm.shape[3]
    ffn = wd_hbm.shape[1]
    tok = do_hbm.shape[0]
    half = tok // 2
    rows = n * cap
    pairs = n // 2
    steps = 2 * (pairs - 1)
    me, sib, nxt, src = peers(n)

    def remote(s, d, ss, rs, dev):
        return pltpu.make_async_remote_copy(src_ref=s, dst_ref=d, send_sem=ss, recv_sem=rs,
                                            device_id={'ep': dev}, device_id_type=pl.DeviceIdType.MESH)

    barrier = pltpu.get_barrier_semaphore()

    @pl.loop(1, n)
    def _(i):
        pl.semaphore_signal(barrier, inc=1, device_id={'ep': (me + i) % n}, device_id_type=pl.DeviceIdType.MESH)

    own_load = pltpu.make_async_copy(do_hbm, gbuf.at[0], g_sem)
    own_load.start()

    def x_load(k):
        r = pl.ds(pl.multiple_of(k * cap, 32), cap)
        return pltpu.make_async_copy(x_hbm.at[src(k)], xbuf.at[:, r, :], x_sem.at[k])

    def w_loads(e):
        return (pltpu.make_async_copy(wg_hbm.at[e], wgu.at[e, :, pl.ds(0, ffn)], w_sem.at[e, 0]),
                pltpu.make_async_copy(wu_hbm.at[e], wgu.at[e, :, pl.ds(ffn, ffn)], w_sem.at[e, 1]),
                pltpu.make_async_copy(wd_hbm.at[e], wd.at[e], w_sem.at[e, 2]))

    tile_src = 4
    for k in range(tile_src):
        x_load(k).start()
    for c in w_loads(0):
        c.start()

    pad = ((0, 0), (0, rt_src.shape[2] - tok))
    slot1 = jnp.pad(slot_ref[...].astype(F32) + 1.0, pad)
    eid = jnp.pad(eid_ref[...], pad)
    gate = jnp.pad(gate_ref[...], pad)
    for e in range(n * e_loc):
        hit = eid == e
        rt_src[e // e_loc, pl.ds(e % e_loc, 1), :] = jnp.sum(jnp.where(hit, slot1, 0.0), axis=0, keepdims=True) - 1.0
        rt_src[e // e_loc, pl.ds(e_loc + e % e_loc, 1), :] = jnp.sum(jnp.where(hit, gate, 0.0), axis=0, keepdims=True)

    own_load.wait()
    pl.semaphore_wait(barrier, n - 1)

    def chunk(k, m):
        return gbuf.at[k, pl.ds(pl.multiple_of((m % 2) * half, 32), half), :]

    def ring_copy(m, k_from):
        return remote(chunk(k_from, m), chunk(2 + 2 * (m // 2), m), ring_s.at[m], ring_r.at[m], nxt)

    def sib_copy(m):
        k = 2 + 2 * (m // 2)
        return remote(chunk(k, m), chunk(k + 1, m), sib_s.at[m], sib_r.at[m], sib)

    own_copy = remote(gbuf.at[0], gbuf.at[1], own_s, own_r, sib)
    for m in range(2):
        ring_copy(m, 0).start()
    own_copy.start()

    def comm(m):
        k = 2 + 2 * (m // 2)
        ring_copy(m, k).wait_recv()
        if isinstance(m, int):
            if m + 4 < steps:
                ring_copy(m + 4, k).start()
        else:
            @pl.when(m + 4 < steps)
            def _():
                ring_copy(m + 4, k).start()
        sib_copy(m).start()

    def route_copy(i):
        return remote(rt_src.at[(me + i) % n], rt_dst.at[me], rt_s.at[i], rt_r.at[i], (me + i) % n)

    tile = tile_src * cap
    n_tiles = rows // tile

    def phase_a(e, t):
        r = pl.ds(pl.multiple_of(t * tile, 128), tile)
        xt = xbuf[e, r, :]
        for c in range(ffn // MXU):
            cols = pl.ds(c * MXU, MXU)
            a = dot(xt, wgu[e, :, cols], 1, 0)
            b = dot(xt, wgu[e, :, pl.ds(ffn + c * MXU, MXU)], 1, 0)
            sg = jax.nn.sigmoid(a)
            silu = a * sg
            hbuf[e, r, cols] = (silu * b).astype(BF16)
            qbuf[e, r, cols] = silu
            pbuf[e, r, cols] = b * sg * (1.0 + a * (1.0 - sg))
        ht = hbuf[e, r, :]
        for c in range(dim // MXU):
            cols = pl.ds(c * MXU, MXU)
            ybuf[e, r, cols] = dot(ht, wd[e, :, cols], 1, 0).astype(BF16)

    def a_wait(i):
        e, t = i % e_loc, i // e_loc

        @pl.when(e == 0)
        def _():
            for j in range(tile_src):
                x_load(t * tile_src + j).wait()

        @pl.when(t == 0)
        def _():
            for c in w_loads(e):
                c.wait()

    a_wait(0)
    for e in range(1, e_loc):
        for c in w_loads(e):
            c.start()
    for k in range(tile_src, n):
        x_load(k).start()
    phase_a(0, 0)
    own_copy.wait_recv()
    for m in range(2, 4):
        ring_copy(m, 1).start()

    @pl.loop(1, n)
    def _(i):
        route_copy(i).start()
    rt_dst[me] = rt_src[me]

    @pl.loop(1, n_tiles * e_loc)
    def _(i):
        a_wait(i)
        phase_a(i % e_loc, i // e_loc)

        @pl.when(i % 3 != 0)
        def _():
            comm((2 * i - 1) // 3)
    done_m = (2 * (n_tiles * e_loc - 1) - 1) // 3 + 1

    @pl.loop(1, n)
    def _(i):
        route_copy(i).wait_recv()

    wide = rt_dst.shape[2]
    slot_no = lax.broadcasted_iota(jnp.int32, (cap, wide), 0).astype(F32)

    def lanes_sum(v):
        parts = [v[:, i:i + LANES] for i in range(0, v.shape[1], LANES)]
        return functools.reduce(jnp.add, parts)

    def select_rows(k):
        s = src(k)
        r = pl.ds(pl.multiple_of(k * cap, 32), cap)
        rt = rt_dst[s]
        hits = [slot_no == rt[e:e + 1, :] for e in range(e_loc)]
        gcols = [jnp.sum(lanes_sum(jnp.where(hits[e], rt[e_loc + e:e_loc + e + 1, :], 0.0)), axis=1, keepdims=True)
                 for e in range(e_loc)]
        onehot = jnp.concatenate([jnp.where(h, 1.0, 0.0).astype(BF16)[:, :tok] for h in hits], axis=0)
        dots = [jnp.zeros((cap, LANES), F32) for _ in range(e_loc)]
        for c in range(dim // MXU):
            cols = pl.ds(c * MXU, MXU)
            o = dot(onehot, gbuf[k, :, cols], 1, 0)
            for e in range(e_loc):
                oe = o[e * cap:(e + 1) * cap, :]
                dots[e] = dots[e] + lanes_sum(oe * ybuf[e, r, cols].astype(F32))
                ybuf[e, r, cols] = (oe * gcols[e]).astype(BF16)
        for e in range(e_loc):
            dot_col = jnp.sum(dots[e], axis=1, keepdims=True)
            gg_src[k, pl.ds(e, 1), :] = jnp.sum(jnp.where(hits[e], dot_col, 0.0), axis=0, keepdims=True)

    def gg_copy(k):
        s = src(k)
        off = (s - me + n) % n
        return remote(gg_src.at[k], gg_dst.at[me], gg_s.at[off], gg_r.at[off], s)

    def gg_send(k0, k1):
        for k in range(k0, k1):
            if k == 0:
                gg_dst[me] = gg_src[0]
            else:
                gg_copy(k).start()

    def hidden_grads(e, r0, r1):
        r = pl.ds(r0, r1 - r0)
        dy = ybuf[e, r, :]
        for c in range(ffn // MXU):
            cols = pl.ds(c * MXU, MXU)
            dh = dot(dy, wd[e, cols, :], 1, 1).astype(BF16).astype(F32)
            dab[e, r, cols] = (dh * pbuf[e, r, cols]).astype(BF16)
            dab[e, r, pl.ds(ffn + c * MXU, MXU)] = (dh * qbuf[e, r, cols]).astype(BF16)

    def weight_grad(lhs, rhs, acc, out, w0, w1, e):
        r = pl.ds(w0, w1 - w0)
        g = dot(lhs[e, r, :], rhs[e, r, :], 0, 0)
        if w0 > 0:
            g = g + acc[e]
        if w1 == rows:
            out[e, pl.ds(0, g.shape[0]), :] = g.astype(BF16)
        else:
            acc[e] = g

    def x_grad(e, r0, r1):
        r = pl.ds(r0, r1 - r0)
        da = dab[e, r, :]
        for c in range(dim // MXU):
            ybuf[e, r, pl.ds(c * MXU, MXU)] = dot(da, wgu[e, pl.ds(c * MXU, MXU), :], 1, 1).astype(BF16)

    next_m = [done_m]

    def comm_next(count=1):
        for _ in range(count):
            if next_m[0] < steps:
                comm(next_m[0])
                next_m[0] += 1

    kept = x_grad_rows(rows)
    stages = [(0, 3, 0, 512), (3, 5, 512, 768), (5, 7, 768, 1280), (7, 8, 1280, 1536)]
    for p0, p1, w0, w1 in stages:
        need = 2 * (p1 - 1)
        if next_m[0] < need:
            comm_next(need - next_m[0])
        for p in range(max(p0, 1), p1):
            for m in (2 * p - 2, 2 * p - 1):
                sib_copy(m).wait_recv()

        for k in range(2 * p0, 2 * p1):
            select_rows(k)
        comm_next()

        for e in range(e_loc):
            hidden_grads(e, 2 * p0 * cap, 2 * p1 * cap)
        gg_send(2 * p0, 2 * p1)
        comm_next()

        @pl.loop(0, e_loc)
        def _(e):
            weight_grad(hbuf, ybuf, acc_d, wd, w0, w1, e)
        comm_next()

        if w1 <= kept:
            for e in range(e_loc):
                x_grad(e, w0, w1)
        comm_next()

        @pl.loop(0, e_loc)
        def _(e):
            weight_grad(xbuf, dab, acc_gu, xbuf, w0, w1, e)
        comm_next()

    @pl.loop(1, n)
    def _(k):
        gg_copy(k).wait_recv()
        gg_copy(k).wait_send()
        route_copy(k).wait_send()
    for m in range(steps):
        ring_copy(m, 0).wait_send()
        sib_copy(m).wait_send()
    own_copy.wait_send()
    gg_out[...] = gg_dst[...]


def x_grad_rows(rows):
    return rows // 2


def write_kernel(n, ybuf, xbuf, wgu, wd, dab, gg, eid_ref, gx_hbm, gwg_hbm, gwu_hbm, gwd_hbm, gate_out,
                 obuf, y_sem, w_sem):
    cap, dim = gx_hbm.shape[2], gx_hbm.shape[3]
    e_loc, ffn = wd.shape[0], wd.shape[1]
    kept = x_grad_rows(n * cap)
    _, _, _, src = peers(n)

    def put(buf, row, k):
        return pltpu.make_async_copy(buf.at[:, pl.ds(row, cap), :], gx_hbm.at[src(k)], y_sem.at[k])

    copies = [put(ybuf, k * cap, k) for k in range(kept // cap)]
    copies += [pltpu.make_async_copy(xbuf.at[:, pl.ds(0, dim), pl.ds(0, ffn)], gwg_hbm, w_sem.at[0]),
               pltpu.make_async_copy(xbuf.at[:, pl.ds(0, dim), pl.ds(ffn, ffn)], gwu_hbm, w_sem.at[1]),
               pltpu.make_async_copy(wd, gwd_hbm, w_sem.at[2])]
    for c in copies:
        c.start()
    tile = (n * cap - kept) // 2
    for t in range(2):
        for e in range(e_loc):
            da = dab[e, pl.ds(kept + t * tile, tile), :]
            for c in range(dim // MXU):
                obuf[e, pl.ds(t * tile, tile), pl.ds(c * MXU, MXU)] = dot(
                    da, wgu[e, pl.ds(c * MXU, MXU), :], 1, 1).astype(BF16)
        for k in range((kept + t * tile) // cap, (kept + (t + 1) * tile) // cap):
            c = put(obuf, k * cap - kept, k)
            c.start()
            copies.append(c)
    eid = eid_ref[...]
    out = jnp.zeros(eid.shape, F32)
    for e in range(n * e_loc):
        out = out + jnp.where(eid == e, gg[e // e_loc, pl.ds(e % e_loc, 1), pl.ds(0, eid.shape[1])], 0.0)
    gate_out[...] = out
    for c in copies:
        c.wait()


def solution(mesh):
    n = mesh.shape['ep']

    def local_step(x_disp, w_gate, w_up, w_down, d_out, slot_idx, expert_id, gate_wt):
        _, e_loc, cap, dim = x_disp.shape
        ffn = w_down.shape[1]
        tok, top_k = slot_idx.shape
        rows = n * cap
        wide = pl.cdiv(tok, LANES) * LANES
        steps = 2 * (n // 2 - 1)
        slot_t, eid_t, gate_t = slot_idx.T, expert_id.T, gate_wt.T
        vmem = pl.BlockSpec(memory_space=pltpu.VMEM)
        hbm = pl.BlockSpec(memory_space=pl.ANY)
        dma = pltpu.SemaphoreType.DMA
        ybuf, xbuf, wgu, wd, dab, gg = pl.pallas_call(
            functools.partial(main_kernel, n),
            out_shape=(pltpu.VMEM((e_loc, rows, dim), BF16),
                       pltpu.VMEM((e_loc, rows, dim), BF16),
                       pltpu.VMEM((e_loc, dim, 2 * ffn), BF16),
                       pltpu.VMEM((e_loc, ffn, dim), BF16),
                       pltpu.VMEM((e_loc, rows, 2 * ffn), BF16),
                       pltpu.VMEM((n, e_loc, wide), F32)),
            in_specs=[hbm] * 5 + [vmem] * 3,
            out_specs=[vmem] * 6,
            scratch_shapes=[
                pltpu.VMEM((n, tok, dim), BF16),
                pltpu.VMEM((e_loc, rows, ffn), F32),
                pltpu.VMEM((e_loc, rows, ffn), F32),
                pltpu.VMEM((e_loc, rows, ffn), BF16),
                pltpu.VMEM((e_loc, dim, 2 * ffn), F32),
                pltpu.VMEM((e_loc, ffn, dim), F32),
                pltpu.VMEM((n, 2 * e_loc, wide), F32),
                pltpu.VMEM((n, 2 * e_loc, wide), F32),
                pltpu.VMEM((n, e_loc, wide), F32),
                pltpu.VMEM((n, e_loc, wide), F32),
                dma((n,)), dma((e_loc, 3)), dma,
                dma((steps,)), dma((steps,)), dma((steps,)), dma((steps,)), dma, dma,
                dma((n,)), dma((n,)), dma((n,)), dma((n,)),
            ],
            compiler_params=pltpu.CompilerParams(collective_id=0, has_side_effects=True,
                                                 vmem_limit_bytes=39 * 1024 * 1024),
            name='experts',
        )(x_disp, w_gate, w_up, w_down, d_out, slot_t, eid_t, gate_t)
        grad_x, grad_wg, grad_wu, grad_wd, gate_out = pl.pallas_call(
            functools.partial(write_kernel, n),
            out_shape=(jax.ShapeDtypeStruct(x_disp.shape, BF16),
                       jax.ShapeDtypeStruct(w_gate.shape, BF16),
                       jax.ShapeDtypeStruct(w_up.shape, BF16),
                       jax.ShapeDtypeStruct(w_down.shape, BF16),
                       jax.ShapeDtypeStruct((top_k, tok), F32)),
            in_specs=[vmem] * 7,
            out_specs=[hbm] * 4 + [vmem],
            scratch_shapes=[pltpu.VMEM((e_loc, rows - x_grad_rows(rows), dim), BF16), dma((n,)), dma((3,))],
            compiler_params=pltpu.CompilerParams(vmem_limit_bytes=8 * 1024 * 1024),
            name='write_out',
        )(ybuf, xbuf, wgu, wd, dab, gg, eid_t)
        return grad_x, grad_wg, grad_wu, grad_wd, gate_out.T

    token_place = P(('dp', 'ep'), None)
    weight_place = P('ep', None, None)
    slot_place = P('dp', 'ep', None, None)
    grad_place = P(('dp', 'ep'), None, None)
    return jax.shard_map(local_step, mesh=mesh,
                         in_specs=(slot_place, weight_place, weight_place, weight_place,
                                   token_place, token_place, token_place, token_place),
                         out_specs=(slot_place, grad_place, grad_place, grad_place, token_place),
                         check_vma=False)
```

```python
import functools

import jax
import jax.numpy as jnp
from jax import lax
from jax.experimental import pallas as pl
from jax.experimental.pallas import tpu as pltpu
from jax.sharding import PartitionSpec as P

F32 = jnp.float32
BF16 = jnp.bfloat16
MXU = 256
LANES = 128


def dot(a, b, ca, cb):
    return lax.dot_general(a, b, (((ca,), (cb,)), ((), ())), preferred_element_type=F32)


def rem(a, b):
    return a % b if isinstance(a, int) else lax.rem(a, jnp.int32(b))


def half_of(a):
    return a // 2 if isinstance(a, int) else lax.div(a, jnp.int32(2))


def peers(n):
    me = lax.axis_index('ep')
    chips = n // 2
    z, core = half_of(me), rem(me, 2)
    sgn = 1 - 2 * core
    sib = z * 2 + 1 - core
    nxt = rem(z + sgn + chips, chips) * 2 + core

    def src(k):
        p, side = half_of(k), rem(k, 2)
        dist = half_of(p + 1)
        chip = rem(z + chips - sgn * (1 - 2 * side) * dist, chips)
        if isinstance(p, int):
            flip = side if p == 0 else side + p + 1
        else:
            flip = side + jnp.where(p == 0, 0, p + 1)
        return chip * 2 + rem(core + flip, 2)

    return me, sib, nxt, src


def main_kernel(n, x_hbm, wg_hbm, wu_hbm, wd_hbm, do_hbm, slot_ref, eid_ref, gate_ref,
                ybuf, xbuf, wgu, wd, dab, gg_out,
                gbuf, pbuf, qbuf, hbuf, acc_gu, acc_d, rt_src, rt_dst, gg_src, gg_dst,
                x_sem, w_sem, g_sem, ring_s, ring_r, sib_s, sib_r, own_s, own_r,
                rt_s, rt_r, gg_s, gg_r):
    e_loc, cap, dim = x_hbm.shape[1], x_hbm.shape[2], x_hbm.shape[3]
    ffn = wd_hbm.shape[1]
    tok = do_hbm.shape[0]
    half = tok // 2
    rows = n * cap
    pairs = n // 2
    steps = 2 * (pairs - 1)
    me, sib, nxt, src = peers(n)

    def remote(s, d, ss, rs, dev):
        return pltpu.make_async_remote_copy(src_ref=s, dst_ref=d, send_sem=ss, recv_sem=rs,
                                            device_id={'ep': dev}, device_id_type=pl.DeviceIdType.MESH)

    barrier = pltpu.get_barrier_semaphore()

    @pl.loop(1, n)
    def _(i):
        pl.semaphore_signal(barrier, inc=1, device_id={'ep': rem(me + i, n)}, device_id_type=pl.DeviceIdType.MESH)

    own_load = pltpu.make_async_copy(do_hbm, gbuf.at[0], g_sem)
    own_load.start()

    def x_load(k):
        r = pl.ds(pl.multiple_of(k * cap, 32), cap)
        return pltpu.make_async_copy(x_hbm.at[src(k)], xbuf.at[:, r, :], x_sem.at[k])

    def w_loads(e):
        return (pltpu.make_async_copy(wg_hbm.at[e], wgu.at[e, :, pl.ds(0, ffn)], w_sem.at[e, 0]),
                pltpu.make_async_copy(wu_hbm.at[e], wgu.at[e, :, pl.ds(ffn, ffn)], w_sem.at[e, 1]),
                pltpu.make_async_copy(wd_hbm.at[e], wd.at[e], w_sem.at[e, 2]))

    tile_src = 4
    for k in range(tile_src):
        x_load(k).start()
    for c in w_loads(0):
        c.start()

    pad = ((0, 0), (0, rt_src.shape[2] - tok))
    slot1 = jnp.pad(slot_ref[...].astype(F32) + 1.0, pad)
    eid = jnp.pad(eid_ref[...], pad)
    gate = jnp.pad(gate_ref[...], pad)
    for e in range(n * e_loc):
        hit = eid == e
        rt_src[e // e_loc, pl.ds(e % e_loc, 1), :] = jnp.sum(jnp.where(hit, slot1, 0.0), axis=0, keepdims=True) - 1.0
        rt_src[e // e_loc, pl.ds(e_loc + e % e_loc, 1), :] = jnp.sum(jnp.where(hit, gate, 0.0), axis=0, keepdims=True)

    def chunk(k, m):
        return gbuf.at[k, pl.ds(pl.multiple_of(rem(m, 2) * half, 32), half), :]

    def ring_copy(m, k_from):
        return remote(chunk(k_from, m), chunk(2 + 2 * half_of(m), m), ring_s.at[m], ring_r.at[m], nxt)

    def sib_copy(m):
        k = 2 + 2 * half_of(m)
        return remote(chunk(k, m), chunk(k + 1, m), sib_s.at[m], sib_r.at[m], sib)

    own_copy = remote(gbuf.at[0], gbuf.at[1], own_s, own_r, sib)
    def comm(m):
        k = 2 + 2 * half_of(m)
        ring_copy(m, k).wait_recv()
        if isinstance(m, int):
            if m + 4 < steps:
                ring_copy(m + 4, k).start()
        else:
            @pl.when(m + 4 < steps)
            def _():
                ring_copy(m + 4, k).start()
        sib_copy(m).start()

    def route_copy(i):
        return remote(rt_src.at[rem(me + i, n)], rt_dst.at[me], rt_s.at[i], rt_r.at[i], rem(me + i, n))

    tile = tile_src * cap
    n_tiles = rows // tile

    def phase_a(e, t):
        r = pl.ds(pl.multiple_of(t * tile, 128), tile)
        xt = xbuf[e, r, :]
        for c in range(ffn // MXU):
            cols = pl.ds(c * MXU, MXU)
            a = dot(xt, wgu[e, :, cols], 1, 0)
            b = dot(xt, wgu[e, :, pl.ds(ffn + c * MXU, MXU)], 1, 0)
            sg = jax.nn.sigmoid(a)
            silu = a * sg
            hbuf[e, r, cols] = (silu * b).astype(BF16)
            qbuf[e, r, cols] = silu
            pbuf[e, r, cols] = b * sg * (1.0 + a * (1.0 - sg))
        ht = hbuf[e, r, :]
        for c in range(dim // MXU):
            cols = pl.ds(c * MXU, MXU)
            ybuf[e, r, cols] = dot(ht, wd[e, :, cols], 1, 0).astype(BF16)

    def a_wait(i):
        e = rem(i, e_loc)
        t = i // e_loc if isinstance(i, int) else lax.div(i, jnp.int32(e_loc))

        @pl.when(e == 0)
        def _():
            for j in range(tile_src):
                x_load(t * tile_src + j).wait()

        @pl.when(t == 0)
        def _():
            for c in w_loads(e):
                c.wait()

    a_wait(0)
    for e in range(1, e_loc):
        for c in w_loads(e):
            c.start()
    for k in range(tile_src, n):
        x_load(k).start()
    phase_a(0, 0)

    own_load.wait()
    pl.semaphore_wait(barrier, n - 1)
    for m in range(2):
        ring_copy(m, 0).start()
    own_copy.start()
    a_wait(1)
    phase_a(1, 0)
    own_copy.wait_recv()
    for m in range(2, 4):
        ring_copy(m, 1).start()

    @pl.loop(1, n)
    def _(i):
        route_copy(i).start()
    rt_dst[me] = rt_src[me]

    @pl.loop(2, n_tiles * e_loc)
    def _(i):
        a_wait(i)
        phase_a(rem(i, e_loc), lax.div(i, jnp.int32(e_loc)))

        @pl.when((i >= 4) & (i != 5))
        def _():
            comm(lax.div(2 * (i - 4), jnp.int32(3)))

    @pl.loop(1, n)
    def _(i):
        route_copy(i).wait_recv()

    wide = rt_dst.shape[2]
    slot_no = lax.broadcasted_iota(jnp.int32, (cap, wide), 0).astype(F32)

    def lanes_sum(v):
        parts = [v[:, i:i + LANES] for i in range(0, v.shape[1], LANES)]
        return functools.reduce(jnp.add, parts)

    def select_rows(k):
        s = src(k)
        r = pl.ds(pl.multiple_of(k * cap, 32), cap)
        rt = rt_dst[s]
        hits = [slot_no == rt[e:e + 1, :] for e in range(e_loc)]
        gcols = [jnp.sum(lanes_sum(jnp.where(hits[e], rt[e_loc + e:e_loc + e + 1, :], 0.0)), axis=1, keepdims=True)
                 for e in range(e_loc)]
        onehot = jnp.concatenate([jnp.where(h, 1.0, 0.0).astype(BF16)[:, :tok] for h in hits], axis=0)
        dots = [jnp.zeros((cap, LANES), F32) for _ in range(e_loc)]
        for c in range(dim // MXU):
            cols = pl.ds(c * MXU, MXU)
            o = dot(onehot, gbuf[k, :, cols], 1, 0)
            for e in range(e_loc):
                oe = o[e * cap:(e + 1) * cap, :]
                dots[e] = dots[e] + lanes_sum(oe * ybuf[e, r, cols].astype(F32))
                ybuf[e, r, cols] = (oe * gcols[e]).astype(BF16)
        for e in range(e_loc):
            dot_col = jnp.sum(dots[e], axis=1, keepdims=True)
            gg_src[k, pl.ds(e, 1), :] = jnp.sum(jnp.where(hits[e], dot_col, 0.0), axis=0, keepdims=True)

    def gg_copy(k):
        s = src(k)
        off = rem(s - me + n, n)
        return remote(gg_src.at[k], gg_dst.at[me], gg_s.at[off], gg_r.at[off], s)

    def gg_send(k0, k1):
        for k in range(k0, k1):
            if k == 0:
                gg_dst[me] = gg_src[0]
            else:
                gg_copy(k).start()

    def hidden_grads(e, r0, r1):
        r = pl.ds(r0, r1 - r0)
        dy = ybuf[e, r, :]
        for c in range(ffn // MXU):
            cols = pl.ds(c * MXU, MXU)
            dh = dot(dy, wd[e, cols, :], 1, 1).astype(BF16).astype(F32)
            dab[e, r, cols] = (dh * pbuf[e, r, cols]).astype(BF16)
            dab[e, r, pl.ds(ffn + c * MXU, MXU)] = (dh * qbuf[e, r, cols]).astype(BF16)

    def weight_grad(lhs, rhs, acc, out, w0, w1, e):
        r = pl.ds(w0, w1 - w0)
        g = dot(lhs[e, r, :], rhs[e, r, :], 0, 0)
        if w0 > 0:
            g = g + acc[e]
        if w1 == rows:
            out[e, pl.ds(0, g.shape[0]), :] = g.astype(BF16)
        else:
            acc[e] = g

    def x_grad(e, r0, r1):
        r = pl.ds(r0, r1 - r0)
        da = dab[e, r, :]
        for c in range(dim // MXU):
            ybuf[e, r, pl.ds(c * MXU, MXU)] = dot(da, wgu[e, pl.ds(c * MXU, MXU), :], 1, 1).astype(BF16)

    kept = x_grad_rows(rows)

    def sel(*ps):
        for p in ps:
            if p > 0:
                for m in (2 * p - 2, 2 * p - 1):
                    sib_copy(m).wait_recv()
        for p in ps:
            select_rows(2 * p)
            select_rows(2 * p + 1)

    def hid(p0, p1):
        for e in range(e_loc):
            hidden_grads(e, 2 * p0 * cap, 2 * p1 * cap)
            if e == 0:
                gg_send(2 * p0, 2 * p1)

    def wgd(w0, w1):
        @pl.loop(0, e_loc)
        def _(e):
            weight_grad(hbuf, ybuf, acc_d, wd, w0, w1, e)

    def wgx(w0, w1, *ms):
        if len(ms) == e_loc or not ms:
            @pl.loop(0, e_loc)
            def _(e):
                weight_grad(xbuf, dab, acc_gu, xbuf, w0, w1, e)
                if ms:
                    comm(ms[0] + e)
        else:
            for e in range(e_loc):
                weight_grad(xbuf, dab, acc_gu, xbuf, w0, w1, e)
                if e < len(ms):
                    comm(ms[e])

    def gx(e, w0, w1):
        x_grad(e, w0, w1)

    sel(0, 1)
    comm(3)
    hid(0, 2)
    sel(2)
    comm(4)
    hid(2, 3)
    wgd(0, 512)
    wgx(0, 512, 5, 6)
    gx(0, 0, 512)
    comm(7)
    sel(3)
    gx(1, 0, 512)
    comm(8)
    sel(4)
    hid(3, 5)
    comm(9)
    wgd(512, 768)
    wgx(512, 768, 10)
    sel(5)
    gx(0, 512, 768)
    comm(11)
    gx(1, 512, 768)
    sel(6)
    comm(12)
    hid(5, 7)
    wgd(768, 1280)
    wgx(768, 1280, 13)
    sel(7)
    hid(7, 8)
    wgd(1280, rows)

    wgx(1280, rows)

    for m in range(steps):
        ring_copy(m, 0).wait_send()
        sib_copy(m).wait_send()
    own_copy.wait_send()

    @pl.loop(1, n)
    def _(k):
        gg_copy(k).wait_recv()
        gg_copy(k).wait_send()
        route_copy(k).wait_send()
    gg_out[...] = gg_dst[...]


def x_grad_rows(rows):
    return rows // 2


def write_kernel(n, ybuf, xbuf, wgu, wd, dab, gg, eid_ref, gx_hbm, gwg_hbm, gwu_hbm, gwd_hbm, gate_out,
                 obuf, y_sem, w_sem):
    cap, dim = gx_hbm.shape[2], gx_hbm.shape[3]
    e_loc, ffn = wd.shape[0], wd.shape[1]
    kept = x_grad_rows(n * cap)
    _, _, _, src = peers(n)

    def put(buf, row, k):
        return pltpu.make_async_copy(buf.at[:, pl.ds(row, cap), :], gx_hbm.at[src(k)], y_sem.at[k])

    copies = [put(ybuf, k * cap, k) for k in range(kept // cap)]
    copies += [pltpu.make_async_copy(xbuf.at[:, pl.ds(0, dim), pl.ds(0, ffn)], gwg_hbm, w_sem.at[0]),
               pltpu.make_async_copy(xbuf.at[:, pl.ds(0, dim), pl.ds(ffn, ffn)], gwu_hbm, w_sem.at[1]),
               pltpu.make_async_copy(wd, gwd_hbm, w_sem.at[2])]
    for c in copies:
        c.start()
    tile = (n * cap - kept) // 2
    for t in range(2):
        for e in range(e_loc):
            da = dab[e, pl.ds(kept + t * tile, tile), :]
            for c in range(dim // MXU):
                obuf[e, pl.ds(t * tile, tile), pl.ds(c * MXU, MXU)] = dot(
                    da, wgu[e, pl.ds(c * MXU, MXU), :], 1, 1).astype(BF16)
        for k in range((kept + t * tile) // cap, (kept + (t + 1) * tile) // cap):
            c = put(obuf, k * cap - kept, k)
            c.start()
            copies.append(c)
    eid = eid_ref[...]
    out = jnp.zeros(eid.shape, F32)
    for e in range(n * e_loc):
        out = out + jnp.where(eid == e, gg[e // e_loc, pl.ds(e % e_loc, 1), pl.ds(0, eid.shape[1])], 0.0)
    gate_out[...] = out
    for c in copies:
        c.wait()


def solution(mesh):
    n = mesh.shape['ep']

    def local_step(x_disp, w_gate, w_up, w_down, d_out, slot_idx, expert_id, gate_wt):
        _, e_loc, cap, dim = x_disp.shape
        ffn = w_down.shape[1]
        tok, top_k = slot_idx.shape
        rows = n * cap
        wide = pl.cdiv(tok, LANES) * LANES
        steps = 2 * (n // 2 - 1)
        slot_t, eid_t, gate_t = slot_idx.T, expert_id.T, gate_wt.T
        vmem = pl.BlockSpec(memory_space=pltpu.VMEM)
        hbm = pl.BlockSpec(memory_space=pl.ANY)
        dma = pltpu.SemaphoreType.DMA
        ybuf, xbuf, wgu, wd, dab, gg = pl.pallas_call(
            functools.partial(main_kernel, n),
            out_shape=(pltpu.VMEM((e_loc, rows, dim), BF16),
                       pltpu.VMEM((e_loc, rows, dim), BF16),
                       pltpu.VMEM((e_loc, dim, 2 * ffn), BF16),
                       pltpu.VMEM((e_loc, ffn, dim), BF16),
                       pltpu.VMEM((e_loc, rows, 2 * ffn), BF16),
                       pltpu.VMEM((n, e_loc, wide), F32)),
            in_specs=[hbm] * 5 + [vmem] * 3,
            out_specs=[vmem] * 6,
            scratch_shapes=[
                pltpu.VMEM((n, tok, dim), BF16),
                pltpu.VMEM((e_loc, rows, ffn), F32),
                pltpu.VMEM((e_loc, rows, ffn), F32),
                pltpu.VMEM((e_loc, rows, ffn), BF16),
                pltpu.VMEM((e_loc, dim, 2 * ffn), F32),
                pltpu.VMEM((e_loc, ffn, dim), F32),
                pltpu.VMEM((n, 2 * e_loc, wide), F32),
                pltpu.VMEM((n, 2 * e_loc, wide), F32),
                pltpu.VMEM((n, e_loc, wide), F32),
                pltpu.VMEM((n, e_loc, wide), F32),
                dma((n,)), dma((e_loc, 3)), dma,
                dma((steps,)), dma((steps,)), dma((steps,)), dma((steps,)), dma, dma,
                dma((n,)), dma((n,)), dma((n,)), dma((n,)),
            ],
            compiler_params=pltpu.CompilerParams(collective_id=0, has_side_effects=True,
                                                 vmem_limit_bytes=39 * 1024 * 1024),
            name='experts',
        )(x_disp, w_gate, w_up, w_down, d_out, slot_t, eid_t, gate_t)
        grad_x, grad_wg, grad_wu, grad_wd, gate_out = pl.pallas_call(
            functools.partial(write_kernel, n),
            out_shape=(jax.ShapeDtypeStruct(x_disp.shape, BF16),
                       jax.ShapeDtypeStruct(w_gate.shape, BF16),
                       jax.ShapeDtypeStruct(w_up.shape, BF16),
                       jax.ShapeDtypeStruct(w_down.shape, BF16),
                       jax.ShapeDtypeStruct((top_k, tok), F32)),
            in_specs=[vmem] * 7,
            out_specs=[hbm] * 4 + [vmem],
            scratch_shapes=[pltpu.VMEM((e_loc, rows - x_grad_rows(rows), dim), BF16), dma((n,)), dma((3,))],
            compiler_params=pltpu.CompilerParams(vmem_limit_bytes=8 * 1024 * 1024),
            name='write_out',
        )(ybuf, xbuf, wgu, wd, dab, gg, eid_t)
        return grad_x, grad_wg, grad_wu, grad_wd, gate_out.T

    token_place = P(('dp', 'ep'), None)
    weight_place = P('ep', None, None)
    slot_place = P('dp', 'ep', None, None)
    grad_place = P(('dp', 'ep'), None, None)
    return jax.shard_map(local_step, mesh=mesh,
                         in_specs=(slot_place, weight_place, weight_place, weight_place,
                                   token_place, token_place, token_place, token_place),
                         out_specs=(slot_place, grad_place, grad_place, grad_place, token_place),
                         check_vma=False)
```

```python
import functools

import jax
import jax.numpy as jnp
from jax import lax
from jax.experimental import pallas as pl
from jax.experimental.pallas import tpu as pltpu
from jax.sharding import PartitionSpec as P

F32 = jnp.float32
BF16 = jnp.bfloat16
MXU = 256
LANES = 128


def dot(a, b, ca, cb):
    return lax.dot_general(a, b, (((ca,), (cb,)), ((), ())), preferred_element_type=F32)


def rem(a, b):
    return a % b if isinstance(a, int) else lax.rem(a, jnp.int32(b))


def half_of(a):
    return a // 2 if isinstance(a, int) else lax.div(a, jnp.int32(2))


def peers(n):
    me = lax.axis_index('ep')
    chips = n // 2
    z, core = half_of(me), rem(me, 2)
    sgn = 1 - 2 * core
    sib = z * 2 + 1 - core
    nxt = rem(z + sgn + chips, chips) * 2 + core

    def src(k):
        p, side = half_of(k), rem(k, 2)
        dist = half_of(p + 1)
        chip = rem(z + chips - sgn * (1 - 2 * side) * dist, chips)
        if isinstance(p, int):
            flip = side if p == 0 else side + p + 1
        else:
            flip = side + jnp.where(p == 0, 0, p + 1)
        return chip * 2 + rem(core + flip, 2)

    return me, sib, nxt, src


def main_kernel(n, x_hbm, wg_hbm, wu_hbm, wd_hbm, do_hbm, slot_ref, eid_ref, gate_ref,
                ybuf, xbuf, wgu, wd, dab, gg_out,
                gbuf, pbuf, qbuf, hbuf, acc_gu, acc_d, rt_src, rt_dst, gg_src, gg_dst,
                x_sem, w_sem, g_sem, ring_s, ring_r, sib_s, sib_r, own_r,
                rt_s, rt_r, gg_s, gg_r):
    e_loc, cap, dim = x_hbm.shape[1], x_hbm.shape[2], x_hbm.shape[3]
    ffn = wd_hbm.shape[1]
    tok = do_hbm.shape[0]
    half = tok // 2
    rows = n * cap
    pairs = n // 2
    steps = 2 * (pairs - 1)
    me, sib, nxt, src = peers(n)

    def remote(s, d, ss, rs, dev):
        return pltpu.make_async_remote_copy(src_ref=s, dst_ref=d, send_sem=ss, recv_sem=rs,
                                            device_id={'ep': dev}, device_id_type=pl.DeviceIdType.MESH)

    barrier = pltpu.get_barrier_semaphore()

    @pl.loop(1, n)
    def _(i):
        pl.semaphore_signal(barrier, inc=1, device_id={'ep': rem(me + i, n)}, device_id_type=pl.DeviceIdType.MESH)

    own_load = pltpu.make_async_copy(do_hbm, gbuf.at[0], g_sem)
    own_load.start()

    def x_load(k):
        r = pl.ds(pl.multiple_of(k * cap, 32), cap)
        return pltpu.make_async_copy(x_hbm.at[src(k)], xbuf.at[:, r, :], x_sem.at[k])

    def w_loads(e):
        return (pltpu.make_async_copy(wg_hbm.at[e], wgu.at[e, :, pl.ds(0, ffn)], w_sem.at[e, 0]),
                pltpu.make_async_copy(wu_hbm.at[e], wgu.at[e, :, pl.ds(ffn, ffn)], w_sem.at[e, 1]),
                pltpu.make_async_copy(wd_hbm.at[e], wd.at[e], w_sem.at[e, 2]))

    tile_src = 4
    for k in range(tile_src):
        x_load(k).start()
    for c in w_loads(0):
        c.start()

    pad = ((0, 0), (0, rt_src.shape[2] - tok))
    slot1 = jnp.pad(slot_ref[...].astype(F32) + 1.0, pad)
    eid = jnp.pad(eid_ref[...], pad)
    gate = jnp.pad(gate_ref[...], pad)
    for e in range(n * e_loc):
        hit = eid == e
        rt_src[e // e_loc, pl.ds(e % e_loc, 1), :] = jnp.sum(jnp.where(hit, slot1, 0.0), axis=0, keepdims=True) - 1.0
        rt_src[e // e_loc, pl.ds(e_loc + e % e_loc, 1), :] = jnp.sum(jnp.where(hit, gate, 0.0), axis=0, keepdims=True)

    def chunk(k, m):
        return gbuf.at[k, pl.ds(pl.multiple_of(rem(m, 2) * half, 32), half), :]

    def ring_copy(m, k_from):
        return remote(chunk(k_from, m), chunk(2 + 2 * half_of(m), m), ring_s, ring_r.at[m], nxt)

    def sib_copy(m):
        k = 2 + 2 * half_of(m)
        return remote(chunk(k, m), chunk(k + 1, m), sib_s, sib_r.at[m], sib)

    own_copy = remote(gbuf.at[0], gbuf.at[1], sib_s, own_r, sib)
    def comm(m):
        k = 2 + 2 * half_of(m)
        ring_copy(m, k).wait_recv()
        if isinstance(m, int):
            if m + 4 < steps:
                ring_copy(m + 4, k).start()
        else:
            @pl.when(m + 4 < steps)
            def _():
                ring_copy(m + 4, k).start()
        sib_copy(m).start()

    def route_copy(i):
        return remote(rt_src.at[rem(me + i, n)], rt_dst.at[me], rt_s, rt_r, rem(me + i, n))

    tile = tile_src * cap
    n_tiles = rows // tile

    def phase_a(e, t):
        r = pl.ds(pl.multiple_of(t * tile, 128), tile)
        xt = xbuf[e, r, :]
        for c in range(ffn // MXU):
            cols = pl.ds(c * MXU, MXU)
            a = dot(xt, wgu[e, :, cols], 1, 0)
            b = dot(xt, wgu[e, :, pl.ds(ffn + c * MXU, MXU)], 1, 0)
            sg = jax.nn.sigmoid(a)
            silu = a * sg
            hbuf[e, r, cols] = (silu * b).astype(BF16)
            qbuf[e, r, cols] = silu
            pbuf[e, r, cols] = b * sg * (1.0 + a * (1.0 - sg))
        ht = hbuf[e, r, :]
        for c in range(dim // MXU):
            cols = pl.ds(c * MXU, MXU)
            ybuf[e, r, cols] = dot(ht, wd[e, :, cols], 1, 0).astype(BF16)

    def a_wait(i):
        e = rem(i, e_loc)
        t = i // e_loc if isinstance(i, int) else lax.div(i, jnp.int32(e_loc))

        @pl.when(e == 0)
        def _():
            for j in range(tile_src):
                x_load(t * tile_src + j).wait()

        @pl.when(t == 0)
        def _():
            for c in w_loads(e):
                c.wait()

    a_wait(0)
    for e in range(1, e_loc):
        for c in w_loads(e):
            c.start()
    for k in range(tile_src, n):
        x_load(k).start()
    phase_a(0, 0)

    own_load.wait()
    pl.semaphore_wait(barrier, n - 1)
    for m in range(2):
        ring_copy(m, 0).start()
    own_copy.start()
    a_wait(1)
    phase_a(1, 0)
    own_copy.wait_recv()
    for m in range(2, 4):
        ring_copy(m, 1).start()

    @pl.loop(1, n)
    def _(i):
        route_copy(i).start()
    rt_dst[me] = rt_src[me]

    @pl.loop(2, n_tiles * e_loc)
    def _(i):
        a_wait(i)
        phase_a(rem(i, e_loc), lax.div(i, jnp.int32(e_loc)))

        @pl.when((i >= 4) & (i != 5))
        def _():
            comm(lax.div(2 * (i - 4), jnp.int32(3)))

    everyone = pl.ds(0, n - 1)
    all_routes = remote(rt_src.at[everyone], rt_dst.at[everyone], rt_s, rt_r, sib)
    all_routes.wait_recv()

    wide = rt_dst.shape[2]
    slot_no = lax.broadcasted_iota(jnp.int32, (cap, wide), 0).astype(F32)

    def lanes_sum(v):
        parts = [v[:, i:i + LANES] for i in range(0, v.shape[1], LANES)]
        return functools.reduce(jnp.add, parts)

    def select_rows(k):
        s = src(k)
        r = pl.ds(pl.multiple_of(k * cap, 32), cap)
        rt = rt_dst[s]
        hits = [slot_no == rt[e:e + 1, :] for e in range(e_loc)]
        gcols = [jnp.sum(lanes_sum(jnp.where(hits[e], rt[e_loc + e:e_loc + e + 1, :], 0.0)), axis=1, keepdims=True)
                 for e in range(e_loc)]
        onehot = jnp.concatenate([jnp.where(h, 1.0, 0.0).astype(BF16)[:, :tok] for h in hits], axis=0)
        dots = [jnp.zeros((cap, LANES), F32) for _ in range(e_loc)]
        for c in range(dim // MXU):
            cols = pl.ds(c * MXU, MXU)
            o = dot(onehot, gbuf[k, :, cols], 1, 0)
            for e in range(e_loc):
                oe = o[e * cap:(e + 1) * cap, :]
                dots[e] = dots[e] + lanes_sum(oe * ybuf[e, r, cols].astype(F32))
                ybuf[e, r, cols] = (oe * gcols[e]).astype(BF16)
        for e in range(e_loc):
            dot_col = jnp.sum(dots[e], axis=1, keepdims=True)
            gg_src[k, pl.ds(e, 1), :] = jnp.sum(jnp.where(hits[e], dot_col, 0.0), axis=0, keepdims=True)

    def gg_copy(k):
        s = src(k)
        return remote(gg_src.at[k], gg_dst.at[me], gg_s, gg_r, s)

    def gg_send(k0, k1):
        for k in range(k0, k1):
            if k == 0:
                gg_dst[me] = gg_src[0]
            else:
                gg_copy(k).start()

    def hidden_grads(e, r0, r1):
        r = pl.ds(r0, r1 - r0)
        dy = ybuf[e, r, :]
        for c in range(ffn // MXU):
            cols = pl.ds(c * MXU, MXU)
            dh = dot(dy, wd[e, cols, :], 1, 1).astype(BF16).astype(F32)
            dab[e, r, cols] = (dh * pbuf[e, r, cols]).astype(BF16)
            dab[e, r, pl.ds(ffn + c * MXU, MXU)] = (dh * qbuf[e, r, cols]).astype(BF16)

    def weight_grad(lhs, rhs, acc, out, w0, w1, e):
        r = pl.ds(w0, w1 - w0)
        g = dot(lhs[e, r, :], rhs[e, r, :], 0, 0)
        if w0 > 0:
            g = g + acc[e]
        if w1 == rows:
            out[e, pl.ds(0, g.shape[0]), :] = g.astype(BF16)
        else:
            acc[e] = g

    def x_grad(e, r0, r1):
        r = pl.ds(r0, r1 - r0)
        da = dab[e, r, :]
        for c in range(dim // MXU):
            ybuf[e, r, pl.ds(c * MXU, MXU)] = dot(da, wgu[e, pl.ds(c * MXU, MXU), :], 1, 1).astype(BF16)

    kept = x_grad_rows(rows)

    def sel(*ps):
        for p in ps:
            if p > 0:
                for m in (2 * p - 2, 2 * p - 1):
                    sib_copy(m).wait_recv()
        for p in ps:
            select_rows(2 * p)
            select_rows(2 * p + 1)

    def hid(p0, p1):
        for e in range(e_loc):
            hidden_grads(e, 2 * p0 * cap, 2 * p1 * cap)
            if e == 0:
                gg_send(2 * p0, 2 * p1)

    def wgd(w0, w1):
        @pl.loop(0, e_loc)
        def _(e):
            weight_grad(hbuf, ybuf, acc_d, wd, w0, w1, e)

    def wgx(w0, w1, *ms):
        if len(ms) == e_loc or not ms:
            @pl.loop(0, e_loc)
            def _(e):
                weight_grad(xbuf, dab, acc_gu, xbuf, w0, w1, e)
                if ms:
                    comm(ms[0] + e)
        else:
            for e in range(e_loc):
                weight_grad(xbuf, dab, acc_gu, xbuf, w0, w1, e)
                if e < len(ms):
                    comm(ms[e])

    def gx(e, w0, w1):
        x_grad(e, w0, w1)

    sel(0, 1)
    comm(3)
    hid(0, 2)
    sel(2)
    comm(4)
    hid(2, 3)
    wgd(0, 512)
    wgx(0, 512, 5, 6)
    gx(0, 0, 512)
    comm(7)
    sel(3)
    gx(1, 0, 512)
    comm(8)
    sel(4)
    hid(3, 5)
    comm(9)
    wgd(512, 768)
    wgx(512, 768, 10)
    sel(5)
    gx(0, 512, 768)
    comm(11)
    gx(1, 512, 768)
    sel(6)
    comm(12)
    hid(5, 7)
    wgd(768, 1280)
    wgx(768, 1280, 13)
    sel(7)
    hid(7, 8)
    wgd(1280, rows)

    wgx(1280, rows)

    all_routes.wait_send()
    blocks = pl.ds(0, steps // 2)
    remote(gbuf.at[blocks], gbuf.at[blocks], ring_s, own_r, nxt).wait_send()
    blocks = pl.ds(0, pairs)
    remote(gbuf.at[blocks], gbuf.at[blocks], sib_s, own_r, sib).wait_send()
    all_gg = remote(gg_src.at[everyone], gg_dst.at[everyone], gg_s, gg_r, sib)
    all_gg.wait_send()
    all_gg.wait_recv()
    gg_out[...] = gg_dst[...]


def x_grad_rows(rows):
    return rows // 2


def write_kernel(n, ybuf, xbuf, wgu, wd, dab, gg, eid_ref, gx_hbm, gwg_hbm, gwu_hbm, gwd_hbm, gate_out,
                 obuf, y_sem, w_sem):
    cap, dim = gx_hbm.shape[2], gx_hbm.shape[3]
    e_loc, ffn = wd.shape[0], wd.shape[1]
    kept = x_grad_rows(n * cap)
    _, _, _, src = peers(n)

    def put(buf, row, k):
        return pltpu.make_async_copy(buf.at[:, pl.ds(row, cap), :], gx_hbm.at[src(k)], y_sem.at[k])

    copies = [put(ybuf, k * cap, k) for k in range(kept // cap)]
    copies += [pltpu.make_async_copy(xbuf.at[:, pl.ds(0, dim), pl.ds(0, ffn)], gwg_hbm, w_sem.at[0]),
               pltpu.make_async_copy(xbuf.at[:, pl.ds(0, dim), pl.ds(ffn, ffn)], gwu_hbm, w_sem.at[1]),
               pltpu.make_async_copy(wd, gwd_hbm, w_sem.at[2])]
    for c in copies:
        c.start()
    tile = (n * cap - kept) // 2
    for t in range(2):
        for e in range(e_loc):
            da = dab[e, pl.ds(kept + t * tile, tile), :]
            for c in range(dim // MXU):
                obuf[e, pl.ds(t * tile, tile), pl.ds(c * MXU, MXU)] = dot(
                    da, wgu[e, pl.ds(c * MXU, MXU), :], 1, 1).astype(BF16)
        for k in range((kept + t * tile) // cap, (kept + (t + 1) * tile) // cap):
            c = put(obuf, k * cap - kept, k)
            c.start()
            copies.append(c)
    eid = eid_ref[...]
    out = jnp.zeros(eid.shape, F32)
    for e in range(n * e_loc):
        out = out + jnp.where(eid == e, gg[e // e_loc, pl.ds(e % e_loc, 1), pl.ds(0, eid.shape[1])], 0.0)
    gate_out[...] = out
    for c in copies:
        c.wait()


def solution(mesh):
    n = mesh.shape['ep']

    def local_step(x_disp, w_gate, w_up, w_down, d_out, slot_idx, expert_id, gate_wt):
        _, e_loc, cap, dim = x_disp.shape
        ffn = w_down.shape[1]
        tok, top_k = slot_idx.shape
        rows = n * cap
        wide = pl.cdiv(tok, LANES) * LANES
        steps = 2 * (n // 2 - 1)
        slot_t, eid_t, gate_t = slot_idx.T, expert_id.T, gate_wt.T
        vmem = pl.BlockSpec(memory_space=pltpu.VMEM)
        hbm = pl.BlockSpec(memory_space=pl.ANY)
        dma = pltpu.SemaphoreType.DMA
        ybuf, xbuf, wgu, wd, dab, gg = pl.pallas_call(
            functools.partial(main_kernel, n),
            out_shape=(pltpu.VMEM((e_loc, rows, dim), BF16),
                       pltpu.VMEM((e_loc, rows, dim), BF16),
                       pltpu.VMEM((e_loc, dim, 2 * ffn), BF16),
                       pltpu.VMEM((e_loc, ffn, dim), BF16),
                       pltpu.VMEM((e_loc, rows, 2 * ffn), BF16),
                       pltpu.VMEM((n, e_loc, wide), F32)),
            in_specs=[hbm] * 5 + [vmem] * 3,
            out_specs=[vmem] * 6,
            scratch_shapes=[
                pltpu.VMEM((n, tok, dim), BF16),
                pltpu.VMEM((e_loc, rows, ffn), F32),
                pltpu.VMEM((e_loc, rows, ffn), F32),
                pltpu.VMEM((e_loc, rows, ffn), BF16),
                pltpu.VMEM((e_loc, dim, 2 * ffn), F32),
                pltpu.VMEM((e_loc, ffn, dim), F32),
                pltpu.VMEM((n, 2 * e_loc, wide), F32),
                pltpu.VMEM((n, 2 * e_loc, wide), F32),
                pltpu.VMEM((n, e_loc, wide), F32),
                pltpu.VMEM((n, e_loc, wide), F32),
                dma((n,)), dma((e_loc, 3)), dma,
                dma, dma((steps,)), dma, dma((steps,)), dma,
                dma, dma, dma, dma,
            ],
            compiler_params=pltpu.CompilerParams(collective_id=0, has_side_effects=True,
                                                 vmem_limit_bytes=39 * 1024 * 1024),
            name='experts',
        )(x_disp, w_gate, w_up, w_down, d_out, slot_t, eid_t, gate_t)
        grad_x, grad_wg, grad_wu, grad_wd, gate_out = pl.pallas_call(
            functools.partial(write_kernel, n),
            out_shape=(jax.ShapeDtypeStruct(x_disp.shape, BF16),
                       jax.ShapeDtypeStruct(w_gate.shape, BF16),
                       jax.ShapeDtypeStruct(w_up.shape, BF16),
                       jax.ShapeDtypeStruct(w_down.shape, BF16),
                       jax.ShapeDtypeStruct((top_k, tok), F32)),
            in_specs=[vmem] * 7,
            out_specs=[hbm] * 4 + [vmem],
            scratch_shapes=[pltpu.VMEM((e_loc, rows - x_grad_rows(rows), dim), BF16), dma((n,)), dma((3,))],
            compiler_params=pltpu.CompilerParams(vmem_limit_bytes=8 * 1024 * 1024),
            name='write_out',
        )(ybuf, xbuf, wgu, wd, dab, gg, eid_t)
        return grad_x, grad_wg, grad_wu, grad_wd, gate_out.T

    token_place = P(('dp', 'ep'), None)
    weight_place = P('ep', None, None)
    slot_place = P('dp', 'ep', None, None)
    grad_place = P(('dp', 'ep'), None, None)
    return jax.shard_map(local_step, mesh=mesh,
                         in_specs=(slot_place, weight_place, weight_place, weight_place,
                                   token_place, token_place, token_place, token_place),
                         out_specs=(slot_place, grad_place, grad_place, grad_place, token_place),
                         check_vma=False)
```
